32 devices in a mesh: dp: 8 (over z, x), expert: 4 (over y, core).
Axes of the slice: x: 2, y: 2, z: 4, core: 2. Of those that a mesh axis runs over, the one named last changes fastest.
Arguments:
- tokens: bfloat16 [4096, 4096], P(('dp', 'expert')), may hold values from -6 to 6
- select: int32 [4, 128], P(None, ('dp', 'expert')), may hold values from -1 to 127, as said below
- gates: float32 [4, 128], P(None, ('dp', 'expert')), may hold values from 0.1 to 1
- w_gate: bfloat16 [4, 4096, 8192], P('expert', None, 'dp'), may hold values from -0.09375 to 0.09375
- w_up: bfloat16 [4, 4096, 8192], P('expert', None, 'dp'), may hold values from -0.09375 to 0.09375
- w_down: bfloat16 [4, 8192, 4096], P('expert', 'dp'), may hold values from -0.0625 to 0.0625
Outputs:
- mixed: bfloat16 [4096, 4096], P(('dp', 'expert'))
The draws below stay inside these ranges and needn't reach their ends.
Inputs may be any that keep to these rules, and one draw needn't show every extreme that they name: `select`: in each block of 4 slots of a row, the live entries come first, distinct and ascending, below 128, followed by -1; every block holds at least one live entry, and every expert fills all 4 slots of some source device.
All inputs are finite; a program needn't handle non-finite values.
Results may differ from the reference program's by a relative error of at most 0.0085.
Values may be sent and summed in bfloat16 or wider, within the bound.
A program may use at most 64 MiB of HBM per device.

```python
import jax
import jax.numpy as jnp

D = 4096
FF = 8192
TOK_DEV = 128
EXPERTS = 4
SLOT = 4
TOKENS = 4096
DEVICES = 32


def draw_select(key, part):
    keys_all = jax.random.split(jax.random.fold_in(key, 11), EXPERTS * DEVICES)

    def one_block(sub_key):
        chosen = jax.random.permutation(sub_key, TOK_DEV)[:SLOT]
        return jnp.sort(chosen)
    picks = jax.vmap(one_block)(keys_all).reshape(EXPERTS, DEVICES, SLOT)
    counts = jax.random.randint(jax.random.fold_in(key, 7), (EXPERTS, DEVICES), 1, SLOT + 1)
    full_src = (jnp.arange(EXPERTS)[:, None] * 37 + 3) % DEVICES
    counts = jnp.where(jnp.arange(DEVICES)[None, :] == full_src, SLOT, counts)
    slot_pos = jnp.arange(SLOT)
    result = jnp.where(slot_pos[None, None, :] < counts[:, :, None], picks, -1)
    return result.reshape(EXPERTS, DEVICES * SLOT).astype(jnp.int32)


def steps_of(key, dims, cuts, least, top_value):
    def one(axis_at, shards_of):
        draws = jax.random.uniform(jax.random.fold_in(jax.random.fold_in(key, 6), axis_at), (shards_of,), jnp.float32, least / len(cuts), top_value / len(cuts))
        return jnp.repeat(jnp.exp(draws), dims[axis_at] // shards_of).reshape((-1,) + (1,) * (len(dims) - axis_at - 1))

    level = one(*cuts[0])
    for cut in cuts[1:]:
        level = level * one(*cut)
    return level


def bell_draw(own_key, extent, scale, bound, pieces=(), held_as=jnp.bfloat16):
    values = jax.random.normal(own_key, extent, jnp.float32) * scale
    if len(pieces) > 0:
        values = steps_of(own_key, extent, pieces, -0.22, 0.18) * values
    return jnp.clip(values, min=-bound, max=bound).astype(held_as)


def setup_inputs(seed: int = 0) -> dict:
    key_of = jax.random.split(jax.random.key(seed), 7)
    tokens = bell_draw(key_of[0], (TOKENS, D), 1.0, 6.0, ((0, 32),))
    select = draw_select(jax.random.fold_in(key_of[6], 71), 0)
    gates = jnp.clip(0.1 + 0.9 * jax.random.uniform(key_of[2], (EXPERTS, DEVICES * SLOT), jnp.float32) ** steps_of(key_of[2], (EXPERTS, DEVICES * SLOT), ((1, 32),), -0.2, 0.2), 0.1, 1.0)
    w_gate = bell_draw(key_of[3], (EXPERTS, D, FF), D ** -0.5, 0.09375, ((0, 4), (2, 8)))
    w_up = bell_draw(key_of[4], (EXPERTS, D, FF), D ** -0.5, 0.09375, ((0, 4), (2, 8)))
    w_down = bell_draw(key_of[5], (EXPERTS, FF, D), FF ** -0.5, 0.0625, ((0, 4), (1, 8)))
    return {"tokens": tokens, "select": select, "gates": gates, "w_gate": w_gate, "w_up": w_up, "w_down": w_down}


def reference(tokens, select, gates, w_gate, w_up, w_down):
    mixed = jnp.zeros((TOKENS, D), jnp.float32)
    source = (jnp.arange(DEVICES * SLOT) // SLOT).astype(jnp.int32)
    for expert_id in range(EXPERTS):
        index_row = select[expert_id]
        is_live = index_row >= 0
        global_idx = (source * TOK_DEV + jnp.where(is_live, index_row, 0)).astype(jnp.int32)
        sel_rows = jnp.where(is_live[:, None], tokens[global_idx], 0).astype(jnp.bfloat16)
        gate_val = jnp.dot(sel_rows, w_gate[expert_id], preferred_element_type=jnp.float32)
        up_val = jnp.dot(sel_rows, w_up[expert_id], preferred_element_type=jnp.float32)
        hidden = (jax.nn.silu(gate_val) * up_val).astype(jnp.bfloat16)
        expert_out = jnp.dot(hidden, w_down[expert_id], preferred_element_type=jnp.float32).astype(jnp.bfloat16)
        weight_col = jnp.where(is_live, gates[expert_id], 0.0).astype(jnp.float32)
        mixed = mixed.at[global_idx].add(weight_col[:, None] * expert_out.astype(jnp.float32))
    return mixed.astype(jnp.bfloat16)
```

```python
import functools

import jax
import jax.numpy as jnp
from jax import lax
from jax.experimental import pallas as pl
from jax.experimental.pallas import tpu as pltpu
from jax.sharding import PartitionSpec as P

MESH = pl.DeviceIdType.MESH
TILE = 16
F32 = jnp.float32
BF16 = jnp.bfloat16


def log2(n):
    return n.bit_length() - 1


def kernel(
    nd, ne, tok, sel, gat, wg_hbm, wu_hbm, wd_hbm, out,
    wg, wu, wd, sb, ab, x, hid, pb, xr, zb, zr, summed, rb, ob, cmb,
    w_sem, a_send, a_recv, gz_send, gz_recv, gx_send, gx_recv,
    rx_send, rx_recv, rz_send, rz_recv, o_send, o_recv,
):
    inner = x.shape[0]
    outer = x.shape[1]
    rows = x.shape[2]
    slots = sel.shape[1]
    tokens_here = tok.shape[0]
    parts = TILE // slots
    wide = sb.shape[2]
    chunks = pb.shape[0]
    cols = pb.shape[4]
    dp = lax.axis_index("dp")
    ex = lax.axis_index("expert")
    za = dp // inner
    xb = lax.rem(dp, inner)
    other = (inner - 1) - xb

    def at_expert(d):
        return (dp, lax.rem(ex + d, ne))

    def at_outer(d):
        return (lax.rem(za + d, outer) * inner + xb, ex)

    partner = (za * inner + other, ex)

    def remote(src, dst, send, recv, to):
        return pltpu.make_async_remote_copy(
            src_ref=src, dst_ref=dst, send_sem=send, recv_sem=recv,
            device_id=to, device_id_type=MESH,
        )

    barrier = pltpu.get_barrier_semaphore()
    for d in range(1, ne):
        pl.semaphore_signal(barrier, inc=1, device_id=at_expert(d), device_id_type=MESH)
    for d in range(1, outer):
        pl.semaphore_signal(barrier, inc=1, device_id=at_outer(d), device_id_type=MESH)
    if inner > 1:
        pl.semaphore_signal(barrier, inc=1, device_id=partner, device_id_type=MESH)

    loads = [
        pltpu.make_async_copy(h.at[0], v, w_sem.at[i])
        for i, (h, v) in enumerate(((wg_hbm, wg), (wu_hbm, wu), (wd_hbm, wd)))
    ]
    for load in loads:
        load.start()

    packed = ne * TILE
    r_id = lax.broadcasted_iota(jnp.int32, (packed, tokens_here), 0)
    t_id = lax.broadcasted_iota(jnp.int32, (packed, tokens_here), 1)
    r_slot = ((r_id >> log2(TILE)) << log2(slots)) + (r_id & (slots - 1))
    r_part = (r_id & (TILE - 1)) >> log2(slots)
    named = jnp.full((packed, tokens_here), -1, jnp.int32)
    for e in range(ne):
        for s in range(slots):
            named = jnp.where(r_slot == e * slots + s, sel[e, s], named)
    hit = jnp.where(named == t_id, 1.0, 0.0)
    pick = jnp.concatenate(
        [jnp.where(r_part == q, hit, 0.0).astype(BF16) for q in range(parts)], axis=1
    )
    stack = jnp.concatenate([tok[:, q * wide:(q + 1) * wide] for q in range(parts)], axis=0)
    gathered = jnp.dot(pick, stack, preferred_element_type=F32).astype(BF16)
    sb[...] = gathered.reshape(ne, TILE, wide)
    ab[ex] = sb[ex]

    pl.semaphore_wait(barrier, (ne - 1) + (outer - 1) + (1 if inner > 1 else 0))

    a_copies = []
    for d in range(1, ne):
        to = at_expert(d)
        copy = remote(sb.at[to[1]], ab.at[ex], a_send.at[d], a_recv.at[d], to)
        copy.start()
        a_copies.append(copy)

    c_id = lax.broadcasted_iota(jnp.int32, (tokens_here, packed), 1)
    n_id = lax.broadcasted_iota(jnp.int32, (tokens_here, packed), 0)
    c_slot = ((c_id >> log2(TILE)) << log2(slots)) + (c_id & (slots - 1))
    weight = jnp.zeros((tokens_here, packed), F32)
    for e in range(ne):
        for s in range(slots):
            weight = jnp.where((c_slot == e * slots + s) & (n_id == sel[e, s]), gat[e, s], weight)
    left = weight
    for i in range(3):
        term = left.astype(BF16)
        cmb[i] = term
        left = left - term.astype(F32)

    u_r = lax.broadcasted_iota(jnp.int32, (packed, parts * rows), 0)
    u_k = lax.broadcasted_iota(jnp.int32, (packed, parts * rows), 1)
    u_col = (
        ((u_r & (TILE - 1)) >> log2(slots)) * rows
        + ((u_r >> log2(TILE)) << log2(slots)) + (u_r & (slots - 1))
    )
    pack = jnp.where(u_k == u_col, 1.0, 0.0).astype(BF16)
    v_r = lax.broadcasted_iota(jnp.int32, (parts * rows, packed), 0)
    v_k = lax.broadcasted_iota(jnp.int32, (parts * rows, packed), 1)
    v_row = (
        ((v_k & (TILE - 1)) >> log2(slots)) * rows
        + ((v_k >> log2(TILE)) << log2(slots)) + (v_k & (slots - 1))
    )
    unpack = jnp.where(v_r == v_row, 1.0, 0.0).astype(BF16)

    for d in range(1, ne):
        src = lax.rem(ex + ne - d, ne)
        remote(sb.at[src], ab.at[src], a_send.at[d], a_recv.at[d], at_expert(d)).wait_recv()
    mine = jnp.dot(unpack, ab[...].reshape(packed, wide), preferred_element_type=F32).astype(BF16)
    for q in range(parts):
        x[xb, za, :, q * wide:(q + 1) * wide] = mine[q * rows:(q + 1) * rows]

    own = x.at[xb, za]
    z_copies = []
    for d in range(1, outer):
        copy = remote(own, own, gz_send.at[d], gz_recv.at[d], at_outer(d))
        copy.start()
        z_copies.append(copy)
    x_copies = []

    def forward(d):
        block = x.at[xb, lax.rem(za + outer - d, outer)]
        copy = remote(block, block, gx_send.at[d], gx_recv.at[d], partner)
        copy.start()
        x_copies.append(copy)

    order = sorted(range(1, outer), key=lambda d: (min(d, outer - d), d))
    if inner > 1:
        forward(0)
    for d in order:
        block = x.at[xb, lax.rem(za + outer - d, outer)]
        remote(block, block, gz_send.at[d], gz_recv.at[d], at_outer(d)).wait_recv()
        if inner > 1:
            forward(d)
    if inner > 1:
        for d in [0] + order:
            block = x.at[other, lax.rem(za + outer - d, outer)]
            remote(block, block, gx_send.at[d], gx_recv.at[d], partner).wait_recv()

    loads[0].wait()
    loads[1].wait()
    total_rows = inner * outer * rows
    step = min(256, hid.shape[1])

    @pl.loop(0, hid.shape[1] // step)
    def _(i):
        at = pl.ds(pl.multiple_of(i * step, step), step)
        block = x[...].reshape(total_rows, x.shape[3])
        g = jnp.dot(block, wg[:, at], preferred_element_type=F32)
        u = jnp.dot(block, wu[:, at], preferred_element_type=F32)
        hid[:, at] = (g / (1.0 + jnp.exp(-g)) * u).astype(BF16)

    loads[2].wait()

    def rx(c):
        return remote(pb.at[c, other], xr.at[c], rx_send.at[c], rx_recv.at[c], partner)

    @pl.loop(0, chunks)
    def _(c):
        at = pl.ds(pl.multiple_of(c * cols, cols), cols)
        part = jnp.dot(hid[...], wd[:, at], preferred_element_type=F32)
        pb[c] = part.astype(BF16).reshape(inner, outer, rows, cols)
        if inner > 1:
            rx(c).start()

    def rz(c, d):
        to = lax.rem(za + d, outer)
        return remote(zb.at[c, to], zr.at[c, d - 1], rz_send.at[c, d], rz_recv.at[c, d], at_outer(d))

    @pl.loop(0, chunks)
    def _(c):
        value = pb[c, xb].astype(F32)
        if inner > 1:
            rx(c).wait_recv()
            value = value + xr[c].astype(F32)
        zb[c] = value.astype(BF16)
        for d in range(1, outer):
            rz(c, d).start()

    per = wide // cols
    for c in range(chunks):
        value = zb[c, za].astype(F32)
        for d in range(1, outer):
            rz(c, d).wait_recv()
            value = value + zr[c, d - 1].astype(F32)
        at = (c % per) * cols
        summed[c // per, :, at:at + cols] = value.astype(BF16)

    back = jnp.dot(pack, summed[...].reshape(parts * rows, wide), preferred_element_type=F32)
    rb[...] = back.astype(BF16).reshape(ne, TILE, wide)
    ob[ex] = rb[ex]
    o_copies = []
    for d in range(1, ne):
        to = at_expert(d)
        copy = remote(rb.at[to[1]], ob.at[ex], o_send.at[d], o_recv.at[d], to)
        copy.start()
        o_copies.append(copy)
    for d in range(1, ne):
        src = lax.rem(ex + ne - d, ne)
        remote(rb.at[src], ob.at[src], o_send.at[d], o_recv.at[d], at_expert(d)).wait_recv()
    got = ob[...].reshape(packed, wide)
    c_part = (c_id & (TILE - 1)) >> log2(slots)
    for q in range(parts):
        total = jnp.zeros((tokens_here, wide), F32)
        for i in range(2, -1, -1):
            coef = jnp.where(c_part == q, cmb[i].astype(F32), 0.0).astype(BF16)
            total = total + jnp.dot(coef, got, preferred_element_type=F32)
        out[:, q * wide:(q + 1) * wide] = total.astype(BF16)

    for copy in a_copies + z_copies + x_copies + o_copies:
        copy.wait_send()

    @pl.loop(0, chunks)
    def _(c):
        if inner > 1:
            rx(c).wait_send()
        for d in range(1, outer):
            rz(c, d).wait_send()


def per_device(nd, ne, tokens, select, gates, w_gate, w_up, w_down):
    tok_dev, width = tokens.shape
    slots = select.shape[1]
    hidden = w_gate.shape[2]
    inner = 2 if nd % 2 == 0 else 1
    outer = nd // inner
    rows = ne * slots
    wide = width * slots // TILE
    parts = TILE // slots
    cols = min(512, wide)
    chunks = width // cols
    vmem = pl.BlockSpec(memory_space=pltpu.VMEM)
    smem = pl.BlockSpec(memory_space=pltpu.SMEM)
    hbm = pl.BlockSpec(memory_space=pl.ANY)
    dma = pltpu.SemaphoreType.DMA
    return pl.pallas_call(
        functools.partial(kernel, nd, ne),
        out_shape=jax.ShapeDtypeStruct((tok_dev, width), BF16),
        in_specs=[vmem, smem, smem, hbm, hbm, hbm],
        out_specs=vmem,
        scratch_shapes=[
            pltpu.VMEM((width, hidden), BF16),
            pltpu.VMEM((width, hidden), BF16),
            pltpu.VMEM((hidden, width), BF16),
            pltpu.VMEM((ne, TILE, wide), BF16),
            pltpu.VMEM((ne, TILE, wide), BF16),
            pltpu.VMEM((inner, outer, rows, width), BF16),
            pltpu.VMEM((nd * rows, hidden), BF16),
            pltpu.VMEM((chunks, inner, outer, rows, cols), BF16),
            pltpu.VMEM((chunks, outer, rows, cols), BF16),
            pltpu.VMEM((chunks, outer, rows, cols), BF16),
            pltpu.VMEM((chunks, max(outer - 1, 1), rows, cols), BF16),
            pltpu.VMEM((parts, rows, wide), BF16),
            pltpu.VMEM((ne, TILE, wide), BF16),
            pltpu.VMEM((ne, TILE, wide), BF16),
            pltpu.VMEM((3, tok_dev, ne * TILE), BF16),
            dma((3,)),
            dma((ne,)), dma((ne,)),
            dma((outer,)), dma((outer,)),
            dma((outer,)), dma((outer,)),
            dma((chunks,)), dma((chunks,)),
            dma((chunks, outer)), dma((chunks, outer)),
            dma((ne,)), dma((ne,)),
        ],
        compiler_params=pltpu.CompilerParams(
            collective_id=0, has_side_effects=True, vmem_limit_bytes=60 * 1024 * 1024
        ),
    )(tokens, select, gates, w_gate, w_up, w_down)


def solution(mesh):
    return jax.shard_map(
        functools.partial(per_device, mesh.shape["dp"], mesh.shape["expert"]),
        mesh=mesh,
        in_specs=(
            P(("dp", "expert"), None),
            P(None, ("dp", "expert")),
            P(None, ("dp", "expert")),
            P("expert", None, "dp"),
            P("expert", None, "dp"),
            P("expert", "dp", None),
        ),
        out_specs=P(("dp", "expert"), None),
        check_vma=False,
    )
```

```python
import functools

import jax
import jax.numpy as jnp
from jax import lax
from jax.experimental import pallas as pl
from jax.experimental.pallas import tpu as pltpu
from jax.sharding import PartitionSpec as P

MESH = pl.DeviceIdType.MESH
TILE = 16
F32 = jnp.float32
BF16 = jnp.bfloat16


def log2(n):
    return n.bit_length() - 1


def kernel(
    nd, ne, tok, sel, gat, wg_hbm, wu_hbm, wd_hbm, out,
    wg, wu, wd, sb, ab, x, g_acc, u_acc, hid, pb, xr, zb, zr, summed, rb, ob, cmb,
    w_sem, a_send, a_recv, gz_send, gz_recv, gx_send, gx_recv,
    rx_send, rx_recv, rz_send, rz_recv, o_send, o_recv,
):
    stages = x.shape[0]
    inner = x.shape[1]
    outer = x.shape[2]
    rows = x.shape[3]
    span = x.shape[4]
    slots = sel.shape[1]
    tokens_here = tok.shape[0]
    parts = TILE // slots
    wide = span // parts
    chunks = pb.shape[0]
    cols = pb.shape[4]
    dp = lax.axis_index("dp")
    ex = lax.axis_index("expert")
    za = dp // inner
    xb = lax.rem(dp, inner)
    other = (inner - 1) - xb

    def at_expert(d):
        return (dp, lax.rem(ex + d, ne))

    def at_outer(d):
        return (lax.rem(za + d, outer) * inner + xb, ex)

    partner = (za * inner + other, ex)

    def remote(src, dst, send, recv, to):
        return pltpu.make_async_remote_copy(
            src_ref=src, dst_ref=dst, send_sem=send, recv_sem=recv,
            device_id=to, device_id_type=MESH,
        )

    barrier = pltpu.get_barrier_semaphore()
    for d in range(1, ne):
        pl.semaphore_signal(barrier, inc=1, device_id=at_expert(d), device_id_type=MESH)
    for d in range(1, outer):
        pl.semaphore_signal(barrier, inc=1, device_id=at_outer(d), device_id_type=MESH)
    if inner > 1:
        pl.semaphore_signal(barrier, inc=1, device_id=partner, device_id_type=MESH)

    loads = [
        pltpu.make_async_copy(h.at[0], v, w_sem.at[i])
        for i, (h, v) in enumerate(((wg_hbm, wg), (wu_hbm, wu), (wd_hbm, wd)))
    ]
    for load in loads:
        load.start()

    packed = ne * TILE
    r_id = lax.broadcasted_iota(jnp.int32, (packed, tokens_here), 0)
    t_id = lax.broadcasted_iota(jnp.int32, (packed, tokens_here), 1)
    r_slot = ((r_id >> log2(TILE)) << log2(slots)) + (r_id & (slots - 1))
    r_part = (r_id & (TILE - 1)) >> log2(slots)
    named = jnp.full((packed, tokens_here), -1, jnp.int32)
    for e in range(ne):
        for s in range(slots):
            named = jnp.where(r_slot == e * slots + s, sel[e, s], named)
    hit = jnp.where(named == t_id, 1.0, 0.0)
    pick = jnp.concatenate(
        [jnp.where(r_part == p, hit, 0.0).astype(BF16) for p in range(parts)], axis=1
    )
    for q in range(stages):
        stack = jnp.concatenate(
            [tok[:, q * span + p * wide:q * span + (p + 1) * wide] for p in range(parts)], axis=0
        )
        gathered = jnp.dot(pick, stack, preferred_element_type=F32).astype(BF16)
        sb[q] = gathered.reshape(ne, TILE, wide)
        ab[q, ex] = sb[q, ex]

    pl.semaphore_wait(barrier, (ne - 1) + (outer - 1) + (1 if inner > 1 else 0))

    sent = []

    def start(copy):
        copy.start()
        sent.append(copy)

    for q in range(stages):
        for d in range(1, ne):
            to = at_expert(d)
            start(remote(sb.at[q, to[1]], ab.at[q, ex], a_send.at[q, d], a_recv.at[q, d], to))

    def packing(shape, packed_dim):
        r = lax.broadcasted_iota(jnp.int32, shape, packed_dim)
        k = lax.broadcasted_iota(jnp.int32, shape, 1 - packed_dim)
        col = (
            ((r & (TILE - 1)) >> log2(slots)) * rows
            + ((r >> log2(TILE)) << log2(slots)) + (r & (slots - 1))
        )
        return jnp.where(k == col, 1.0, 0.0).astype(BF16)

    pack = packing((packed, parts * rows), 0)
    unpack = packing((parts * rows, packed), 1)

    def gx(q, owner_b, d):
        block = x.at[q, owner_b, lax.rem(za + outer - d, outer)]
        return remote(block, block, gx_send.at[q, d], gx_recv.at[q, d], partner)

    def gz(q, d, owner_a):
        block = x.at[q, xb, owner_a]
        return remote(block, block, gz_send.at[q, d], gz_recv.at[q, d], at_outer(d))

    order = sorted(range(1, outer), key=lambda d: (min(d, outer - d), d))
    for q in range(stages):
        for d in range(1, ne):
            src = lax.rem(ex + ne - d, ne)
            remote(
                sb.at[q, src], ab.at[q, src], a_send.at[q, d], a_recv.at[q, d], at_expert(d)
            ).wait_recv()
        mine = jnp.dot(
            unpack, ab[q].reshape(packed, wide), preferred_element_type=F32
        ).astype(BF16)
        for p in range(parts):
            x[q, xb, za, :, p * wide:(p + 1) * wide] = mine[p * rows:(p + 1) * rows]
        for d in order:
            start(gz(q, d, za))
        if inner > 1:
            start(gx(q, xb, 0))

    terms = 3
    c_id = lax.broadcasted_iota(jnp.int32, (tokens_here, terms * packed), 1)
    n_id = lax.broadcasted_iota(jnp.int32, (tokens_here, terms * packed), 0)
    c_row = c_id & (packed - 1)
    c_slot = ((c_row >> log2(TILE)) << log2(slots)) + (c_row & (slots - 1))
    weight = jnp.zeros((tokens_here, terms * packed), F32)
    for e in range(ne):
        for s in range(slots):
            weight = jnp.where((c_slot == e * slots + s) & (n_id == sel[e, s]), gat[e, s], weight)
    left = weight
    coef = jnp.zeros_like(weight)
    for i in range(terms):
        term = left.astype(BF16).astype(F32)
        coef = jnp.where((c_id >> log2(packed)) == i, term, coef)
        left = left - term
    c_part = (c_row & (TILE - 1)) >> log2(slots)
    for p in range(parts):
        cmb[p] = jnp.where(c_part == p, coef, 0.0).astype(BF16)

    total_rows = inner * outer * rows
    step = min(256, hid.shape[1])

    def arrive(q):
        for d in order:
            gz(q, d, lax.rem(za + outer - d, outer)).wait_recv()
            if inner > 1:
                start(gx(q, xb, d))

    def multiply(q):
        if inner > 1:
            for d in [0] + order:
                gx(q, other, d).wait_recv()
        if q == 0:
            loads[0].wait()
            loads[1].wait()

        @pl.loop(0, hid.shape[1] // step)
        def _(i):
            at = pl.ds(pl.multiple_of(i * step, step), step)
            block = x[q].reshape(total_rows, span)
            g = jnp.dot(block, wg[q * span:(q + 1) * span, at], preferred_element_type=F32)
            u = jnp.dot(block, wu[q * span:(q + 1) * span, at], preferred_element_type=F32)
            if q > 0:
                g = g + g_acc[:, at]
                u = u + u_acc[:, at]
            if q < stages - 1:
                g_acc[:, at] = g
                u_acc[:, at] = u
            else:
                hid[:, at] = (g / (1.0 + jnp.exp(-g)) * u).astype(BF16)

    for q in range(stages):
        arrive(q)
        if q > 0:
            multiply(q - 1)
    multiply(stages - 1)

    loads[2].wait()

    def rx(c):
        return remote(pb.at[c, other], xr.at[c], rx_send.at[c], rx_recv.at[c], partner)

    @pl.loop(0, chunks)
    def _(c):
        at = pl.ds(pl.multiple_of(c * cols, cols), cols)
        part = jnp.dot(hid[...], wd[:, at], preferred_element_type=F32)
        pb[c] = part.astype(BF16).reshape(inner, outer, rows, cols)
        if inner > 1:
            rx(c).start()

    def rz(c, d):
        to = lax.rem(za + d, outer)
        return remote(zb.at[c, to], zr.at[c, d - 1], rz_send.at[c, d], rz_recv.at[c, d], at_outer(d))

    def inner_sum(c):
        value = pb[c, xb].astype(F32)
        if inner > 1:
            rx(c).wait_recv()
            value = value + xr[c].astype(F32)
        zb[c] = value.astype(BF16)
        for d in order:
            rz(c, d).start()

    per = span // cols

    def outer_sum(c):
        value = zb[c, za].astype(F32)
        for d in order:
            rz(c, d).wait_recv()
            value = value + zr[c, d - 1].astype(F32)
        for k in range(cols // wide):
            p = (c % per) * (cols // wide) + k
            summed[c // per, p] = value[:, k * wide:(k + 1) * wide].astype(BF16)

    def give(q):
        back = jnp.dot(pack, summed[q].reshape(parts * rows, wide), preferred_element_type=F32)
        rb[q] = back.astype(BF16).reshape(ne, TILE, wide)
        ob[q, ex] = rb[q, ex]
        for d in range(1, ne):
            to = at_expert(d)
            start(remote(rb.at[q, to[1]], ob.at[q, ex], o_send.at[q, d], o_recv.at[q, d], to))

    def mix(q):
        for d in range(1, ne):
            src = lax.rem(ex + ne - d, ne)
            remote(
                rb.at[q, src], ob.at[q, src], o_send.at[q, d], o_recv.at[q, d], at_expert(d)
            ).wait_recv()
        got = ob[q].reshape(packed, wide)
        total = jnp.dot(
            cmb[...].reshape(parts * tokens_here, terms * packed),
            jnp.concatenate([got] * terms, axis=0),
            preferred_element_type=F32,
        ).astype(BF16)
        for p in range(parts):
            at = q * span + p * wide
            out[:, at:at + wide] = total[p * tokens_here:(p + 1) * tokens_here]

    lag = min(3, chunks)
    for c in range(chunks + lag):
        if c < chunks:
            inner_sum(c)
        done = c - lag
        if done >= 0:
            outer_sum(done)
            if done % per == per - 1:
                give(done // per)
                if done // per > 0:
                    mix(done // per - 1)
    mix(stages - 1)

    for copy in sent:
        copy.wait_send()

    @pl.loop(0, chunks)
    def _(c):
        if inner > 1:
            rx(c).wait_send()
        for d in range(1, outer):
            rz(c, d).wait_send()


def per_device(nd, ne, tokens, select, gates, w_gate, w_up, w_down):
    tok_dev, width = tokens.shape
    slots = select.shape[1]
    hidden = w_gate.shape[2]
    inner = 2 if nd % 2 == 0 else 1
    outer = nd // inner
    rows = ne * slots
    parts = TILE // slots
    stages = 4
    span = width // stages
    wide = span // parts
    cols = span // 2
    chunks = width // cols
    vmem = pl.BlockSpec(memory_space=pltpu.VMEM)
    smem = pl.BlockSpec(memory_space=pltpu.SMEM)
    hbm = pl.BlockSpec(memory_space=pl.ANY)
    dma = pltpu.SemaphoreType.DMA
    return pl.pallas_call(
        functools.partial(kernel, nd, ne),
        out_shape=jax.ShapeDtypeStruct((tok_dev, width), BF16),
        in_specs=[vmem, smem, smem, hbm, hbm, hbm],
        out_specs=vmem,
        scratch_shapes=[
            pltpu.VMEM((width, hidden), BF16),
            pltpu.VMEM((width, hidden), BF16),
            pltpu.VMEM((hidden, width), BF16),
            pltpu.VMEM((stages, ne, TILE, wide), BF16),
            pltpu.VMEM((stages, ne, TILE, wide), BF16),
            pltpu.VMEM((stages, inner, outer, rows, span), BF16),
            pltpu.VMEM((nd * rows, hidden), F32),
            pltpu.VMEM((nd * rows, hidden), F32),
            pltpu.VMEM((nd * rows, hidden), BF16),
            pltpu.VMEM((chunks, inner, outer, rows, cols), BF16),
            pltpu.VMEM((chunks, outer, rows, cols), BF16),
            pltpu.VMEM((chunks, outer, rows, cols), BF16),
            pltpu.VMEM((chunks, max(outer - 1, 1), rows, cols), BF16),
            pltpu.VMEM((stages, parts, rows, wide), BF16),
            pltpu.VMEM((stages, ne, TILE, wide), BF16),
            pltpu.VMEM((stages, ne, TILE, wide), BF16),
            pltpu.VMEM((parts, tok_dev, 3 * ne * TILE), BF16),
            dma((3,)),
            dma((stages, ne)), dma((stages, ne)),
            dma((stages, outer)), dma((stages, outer)),
            dma((stages, outer)), dma((stages, outer)),
            dma((chunks,)), dma((chunks,)),
            dma((chunks, outer)), dma((chunks, outer)),
            dma((stages, ne)), dma((stages, ne)),
        ],
        compiler_params=pltpu.CompilerParams(
            collective_id=0, has_side_effects=True, vmem_limit_bytes=60 * 1024 * 1024
        ),
    )(tokens, select, gates, w_gate, w_up, w_down)


def solution(mesh):
    return jax.shard_map(
        functools.partial(per_device, mesh.shape["dp"], mesh.shape["expert"]),
        mesh=mesh,
        in_specs=(
            P(("dp", "expert"), None),
            P(None, ("dp", "expert")),
            P(None, ("dp", "expert")),
            P("expert", None, "dp"),
            P("expert", None, "dp"),
            P("expert", "dp", None),
        ),
        out_specs=P(("dp", "expert"), None),
        check_vma=False,
    )
```
